32 devices in a mesh: wide: 16 (over z, x, core), narrow: 2 (over y).
Axes of the slice: x: 2, y: 2, z: 4, core: 2. Of those that a mesh axis runs over, the one named last changes fastest.
Arguments:
- vectors: float32 [1024, 16384], P('narrow', 'wide'), may hold values from -6 to 6
- weights: bfloat16 [5, 64, 256, 512], P(None, 'wide', 'narrow'), may hold values from -0.25 to 0.25
Outputs:
- transformed: float32 [1024, 16384], P('narrow', 'wide')
The draws below stay inside these ranges and needn't reach their ends.
All inputs are finite; a program needn't handle non-finite values.
Results may differ from the reference program's by a relative error of at most 0.0003.
Values may be sent and summed in bfloat16 or wider, within the bound.
A program may use at most 64 MiB of HBM per device.

```python
import jax
import jax.numpy as jnp
from jax import lax

BLK_DEV = 4
BLOCK = 256
LEVELS = 5
VECTORS = 1024
BLOCKS = 64
COEFFS = 16384
N_WIDE = 16


def steps_of(key, shape, shards, low, top_value):
    gain, own = 1.0, jax.random.fold_in(key, 6)
    for position, shards_of in shards:
        steps = jnp.exp(jax.random.uniform(jax.random.fold_in(own, position), (shards_of,), jnp.float32, low / len(shards), top_value / len(shards)))
        gain = gain * jnp.repeat(steps, shape[position] // shards_of).reshape([-1 if axis == position else 1 for axis in range(len(shape))])
    return gain


def noise(stream_key, dims, spread, limit, shards=(), dtype=jnp.bfloat16):
    level = steps_of(stream_key, dims, shards, -0.22, 0.18) if shards else 1.0
    array = jax.random.normal(stream_key, dims, jnp.float32) * spread * level
    return jnp.minimum(jnp.maximum(array, -limit), limit).astype(dtype)


def setup_inputs(seed: int = 0) -> dict:
    arg_keys = jax.random.split(jax.random.key(seed), 3)
    vectors = noise(arg_keys[0], (VECTORS, COEFFS), 1.0, 6.0, ((0, 2), (1, 16)), jnp.float32)
    weights = noise(arg_keys[1], (LEVELS, BLOCKS, BLOCK, 2 * BLOCK), (2 * BLOCK) ** -0.5, 0.25, ((1, 16), (2, 2)))
    return dict(vectors=vectors, weights=weights)


def apply_level(current, matrices, level_bit):
    columns, block_count, block_size = current.shape
    stride = 1 << level_bit
    grouped = current.reshape(columns, block_count // (2 * stride), 2, stride, block_size)
    paired = jnp.concatenate([grouped[:, :, 0], grouped[:, :, 1]], -1)
    matrix = matrices.astype(jnp.float32).reshape(block_count // (2 * stride), 2, stride, block_size, 2 * block_size)
    result = jnp.einsum('vaji,asjoi->vasjo', paired, matrix, precision=lax.Precision.HIGHEST)
    return result.reshape(columns, block_count, block_size)


def reference(vectors, weights):
    local_bits = BLK_DEV.bit_length() - 1
    wide_top = N_WIDE.bit_length() - 1
    level_bits = [0, 1, local_bits, local_bits + wide_top // 2, local_bits + wide_top - 1]
    block_size = weights.shape[2]
    current = vectors.reshape(vectors.shape[0], vectors.shape[1] // block_size, block_size)
    for level_index in range(LEVELS):
        current = apply_level(current, weights[level_index], level_bits[level_index])
    return current.reshape(vectors.shape)
```

```python
import functools

import jax
import jax.numpy as jnp
from jax import lax
from jax.experimental import pallas as pl
from jax.experimental.pallas import tpu as pltpu
from jax.sharding import PartitionSpec as P

MESH = pl.DeviceIdType.MESH
POWER = 12
TOP = 2.0 ** (126 / POWER)
TINY = 1e-35
TILE = 256
WINDOW = 5
BF16 = jnp.bfloat16
F32 = jnp.float32

WEIGHT_ORDER = (
    (0, 0), (0, 2), (1, 0), (2, 0), (1, 2), (2, 2), (3, 0), (3, 2),
    (0, 1), (0, 3), (1, 1), (2, 1), (1, 3), (2, 3), (3, 1), (3, 3),
    (4, 0), (4, 2), (4, 1), (4, 3),
)
COMPUTE_ORDER = (
    (0, 0), (0, 2), (1, 0), (1, 2), (2, 0), (2, 2), (3, 0), (0, 1), (3, 2), (0, 3),
    (1, 1), (1, 3), (2, 1), (2, 3), (3, 1), (3, 3),
    (4, 0), (4, 2), (4, 1), (4, 3),
)


def split(value):
    high = value.astype(BF16)
    return high, (value - high.astype(F32)).astype(BF16)


def encode(value):
    scale = jnp.maximum(jnp.max(jnp.abs(value), axis=0, keepdims=True), TINY)
    t = value * (TOP / scale)
    t2 = t * t
    t4 = t2 * t2
    t12 = t4 * t4 * t4
    return jnp.where(t < 0, -t12, t12).astype(BF16), scale


def decode(code, scale):
    wide = code.astype(F32)
    size = jnp.exp(jnp.log(jnp.abs(wide)) * (1.0 / POWER)) * (scale * (1.0 / TOP))
    return jnp.where(wide == 0, 0.0, jnp.where(wide < 0, -size, size))


def kernel(
    peers, strides, x_hbm, w_hbm, out_hbm,
    x, w, l0, l1, l1_in, l2, z1_out, z1_in, s1_out, s1_in, l3, z2_out, z2_in, s2_out, s2_in, out,
    x_sem, own_sem, w_send, w_recv, core_send, core_recv, z_send, z_recv, s_send, s_recv, out_sem,
):
    columns = x.shape[0]
    size = w.shape[3] // 2
    rows = w_hbm.shape[2]
    blocks = w.shape[1]
    tiles = columns // TILE
    me_n = lax.axis_index("narrow")
    me_w = lax.axis_index("wide")
    sides = [me_w // stride % 2 for stride in strides]
    partners = [me_w + (1 - 2 * side) * stride for side, stride in zip(sides, strides)]

    def x_copy(half):
        span = pl.ds(half * 2 * size, 2 * size)
        return pltpu.make_async_copy(x_hbm.at[:, span], x.at[:, span], x_sem.at[half])

    def own_copy(level, block):
        span = pl.ds(pl.multiple_of(me_n * rows, rows), rows)
        return pltpu.make_async_copy(
            w_hbm.at[level, block], w.at[level, block, span], own_sem.at[level, block]
        )

    def weight_copy(level, block, k, owner):
        span = pl.ds(pl.multiple_of(owner * rows, rows), rows)
        return pltpu.make_async_remote_copy(
            src_ref=w_hbm.at[level, block],
            dst_ref=w.at[level, block, span],
            send_sem=w_send.at[level, block, k - 1],
            recv_sem=w_recv.at[level, block, k - 1],
            device_id={"narrow": lax.rem(me_n + k, peers)},
            device_id_type=MESH,
        )

    def send_weight(position):
        if position < len(WEIGHT_ORDER):
            level, block = WEIGHT_ORDER[position]
            for k in range(1, peers):
                weight_copy(level, block, k, me_n).start()

    def core_copy(block):
        return pltpu.make_async_remote_copy(
            src_ref=l1.at[block], dst_ref=l1_in.at[block],
            send_sem=core_send.at[block], recv_sem=core_recv.at[block],
            device_id={"wide": partners[0]}, device_id_type=MESH,
        )

    def code_copies(level, block):
        source, target = ((z1_out, z1_in), (z2_out, z2_in))[level]
        s_source, s_target = ((s1_out, s1_in), (s2_out, s2_in))[level]
        partner = partners[level + 1]
        return (
            pltpu.make_async_remote_copy(
                src_ref=s_source.at[block], dst_ref=s_target.at[block],
                send_sem=s_send.at[level, block], recv_sem=s_recv.at[level, block],
                device_id={"wide": partner}, device_id_type=MESH,
            ),
            pltpu.make_async_remote_copy(
                src_ref=source.at[block], dst_ref=target.at[block],
                send_sem=z_send.at[level, block], recv_sem=z_recv.at[level, block],
                device_id={"wide": partner}, device_id_type=MESH,
            ),
        )

    def out_copy(block):
        return pltpu.make_async_copy(
            out.at[block], out_hbm.at[:, pl.ds(block * size, size)], out_sem.at[block]
        )

    def product(level, block, first, second, side, finish):
        def step(tile, carry):
            total = None
            for part, half in ((first, side), (second, 1 - side)):
                start = half * size
                if not isinstance(half, int):
                    start = pl.multiple_of(start, size)
                matrix = w[level, block, :, pl.ds(start, size)]
                lhs = jnp.concatenate(part(tile), axis=0)
                term = lax.dot_general(
                    lhs, matrix, (((1,), (1,)), ((), ())), preferred_element_type=F32
                )
                total = term if total is None else total + term
            finish(tile, total[:TILE] + total[TILE:])
            return carry

        lax.fori_loop(0, tiles, step, 0)

    def at_tile(tile):
        return pl.ds(pl.multiple_of(tile * TILE, TILE), TILE)

    def at_scale(tile):
        return pl.ds(pl.multiple_of(tile * 8, 8), 8)

    def from_x(block):
        return lambda tile: split(x[at_tile(tile), pl.ds(block * size, size)])

    def from_pair(ref, block):
        return lambda tile: (ref[block, 0, at_tile(tile)], ref[block, 1, at_tile(tile)])

    def from_code(ref, scales, block):
        return lambda tile: split(
            decode(ref[block, at_tile(tile)], scales[block, at_scale(tile)][:1])
        )

    def to_pair(ref, block):
        def finish(tile, value):
            high, low = split(value)
            ref[block, 0, at_tile(tile)] = high
            ref[block, 1, at_tile(tile)] = low

        return finish

    def to_code(ref, code_ref, scale_ref, block):
        keep = to_pair(ref, block)

        def finish(tile, value):
            keep(tile, value)
            code, scale = encode(value)
            code_ref[block, at_tile(tile)] = code
            scale_ref[block, at_scale(tile)] = jnp.broadcast_to(scale, (8, size))

        return finish

    def to_out(block):
        def finish(tile, value):
            out[block, at_tile(tile)] = value

        return finish

    for half in range(blocks // 2):
        x_copy(half).start()
    for level, block in WEIGHT_ORDER:
        own_copy(level, block).start()

    barrier = pltpu.get_barrier_semaphore()
    for k in range(1, peers):
        pl.semaphore_signal(
            barrier, inc=1, device_id={"narrow": lax.rem(me_n + k, peers)}, device_id_type=MESH
        )
    for partner in partners:
        pl.semaphore_signal(barrier, inc=1, device_id={"wide": partner}, device_id_type=MESH)
    pl.semaphore_wait(barrier, peers - 1 + len(partners))

    for position in range(WINDOW):
        send_weight(position)

    arrived = [0]

    def need_weight(level, block):
        while (level, block) in WEIGHT_ORDER[arrived[0]:]:
            next_level, next_block = WEIGHT_ORDER[arrived[0]]
            own_copy(next_level, next_block).wait()
            for k in range(1, peers):
                weight_copy(
                    next_level, next_block, k, lax.rem(me_n + peers - k, peers)
                ).wait_recv()
            send_weight(arrived[0] + WINDOW)
            arrived[0] += 1

    x_ready = set()
    for level, block in COMPUTE_ORDER:
        if level == 0 and block // 2 not in x_ready:
            x_copy(block // 2).wait()
            x_ready.add(block // 2)
        need_weight(level, block)
        if level < 2:
            stride = 1 << level
            low = block - block // stride % 2 * stride
            high = low + stride
        if level == 0:
            product(level, block, from_x(low), from_x(high), 0, to_pair(l0, block))
        elif level == 1:
            product(level, block, from_pair(l0, low), from_pair(l0, high), 0, to_pair(l1, block))
            core_copy(block).start()
        elif level == 2:
            core_copy(block).wait_recv()
            product(
                level, block, from_pair(l1, block), from_pair(l1_in, block), sides[0],
                to_code(l2, z1_out, s1_out, block),
            )
            for copy in code_copies(0, block):
                copy.start()
        elif level == 3:
            for copy in code_copies(0, block):
                copy.wait_recv()
            product(
                level, block, from_pair(l2, block), from_code(z1_in, s1_in, block), sides[1],
                to_code(l3, z2_out, s2_out, block),
            )
            for copy in code_copies(1, block):
                copy.start()
        else:
            for copy in code_copies(1, block):
                copy.wait_recv()
            product(
                level, block, from_pair(l3, block), from_code(z2_in, s2_in, block), sides[2],
                to_out(block),
            )
            out_copy(block).start()

    for level, block in WEIGHT_ORDER:
        for k in range(1, peers):
            weight_copy(level, block, k, me_n).wait_send()
    for block in range(blocks):
        core_copy(block).wait_send()
        for level in range(2):
            for copy in code_copies(level, block):
                copy.wait_send()
        out_copy(block).wait()


def on_device(vectors, weights):
    columns, coeffs = vectors.shape
    levels, blocks, rows, depth = weights.shape
    size = depth // 2
    peers = lax.axis_size("narrow")
    wide_top = lax.axis_size("wide").bit_length() - 1
    strides = [1 << bit for bit in (0, wide_top // 2, wide_top - 1)]
    tiles = columns // TILE
    pair = pltpu.VMEM((blocks, 2, columns, size), BF16)
    code = pltpu.VMEM((blocks, columns, size), BF16)
    scale = pltpu.VMEM((blocks, tiles * 8, size), F32)
    dma = pltpu.SemaphoreType.DMA
    return pl.pallas_call(
        functools.partial(kernel, peers, strides),
        out_shape=jax.ShapeDtypeStruct((columns, coeffs), F32),
        in_specs=[pl.BlockSpec(memory_space=pl.ANY)] * 2,
        out_specs=pl.BlockSpec(memory_space=pl.ANY),
        scratch_shapes=[
            pltpu.VMEM((columns, coeffs), F32),
            pltpu.VMEM((levels, blocks, size, depth), BF16),
            pair, pair, pair, pair,
            code, code, scale, scale,
            pair,
            code, code, scale, scale,
            pltpu.VMEM((blocks, columns, size), F32),
            dma((blocks // 2,)),
            dma((levels, blocks)),
            dma((levels, blocks, max(peers - 1, 1))),
            dma((levels, blocks, max(peers - 1, 1))),
            dma((blocks,)),
            dma((blocks,)),
            dma((2, blocks)),
            dma((2, blocks)),
            dma((2, blocks)),
            dma((2, blocks)),
            dma((blocks,)),
        ],
        compiler_params=pltpu.CompilerParams(
            collective_id=0, has_side_effects=True, vmem_limit_bytes=60 * 1024 * 1024
        ),
    )(vectors, weights)


def solution(mesh):
    placed = (P("narrow", "wide"), P(None, "wide", "narrow", None))
    return jax.shard_map(
        on_device, mesh=mesh, in_specs=placed, out_specs=P("narrow", "wide"), check_vma=False
    )
```

```python
import functools

import jax
import jax.numpy as jnp
from jax import lax
from jax.experimental import pallas as pl
from jax.experimental.pallas import tpu as pltpu
from jax.sharding import PartitionSpec as P

MESH = pl.DeviceIdType.MESH
POWER = 12
TOP = 2.0 ** (126 / POWER)
TINY = 1e-35
TILE = 256
WINDOW = 5
BF16 = jnp.bfloat16
F32 = jnp.float32

WEIGHT_ORDER = (
    (0, 0), (0, 2), (1, 0), (2, 0), (1, 2), (2, 2), (3, 0), (0, 1),
    (0, 3), (1, 1), (2, 1), (3, 2), (1, 3), (2, 3), (3, 1), (3, 3),
    (4, 0), (4, 2), (4, 1), (4, 3),
)
COMPUTE_ORDER = (
    (0, 0), (0, 2), (1, 0), (1, 2), (2, 0), (2, 2), (3, 0), (0, 1), (0, 3),
    (1, 1), (2, 1), (3, 2), (1, 3), (2, 3), (3, 1), (3, 3),
    (4, 0), (4, 2), (4, 1), (4, 3),
)


def split(value):
    high = value.astype(BF16)
    return high, (value - high.astype(F32)).astype(BF16)


def encode(value):
    scale = jnp.maximum(jnp.max(jnp.abs(value), axis=0, keepdims=True), TINY)
    t = value * (TOP / scale)
    t2 = t * t
    t4 = t2 * t2
    t12 = t4 * t4 * t4
    return jnp.where(t < 0, -t12, t12).astype(BF16), scale


def decode(code, scale):
    wide = code.astype(F32)
    size = jnp.exp(jnp.log(jnp.abs(wide)) * (1.0 / POWER)) * (scale * (1.0 / TOP))
    return jnp.where(wide == 0, 0.0, jnp.where(wide < 0, -size, size))


def kernel(
    peers, strides, x_hbm, w_hbm, out,
    x, w, l0, l1, l1_in, l2, z1_out, z1_in, s1_out, s1_in, l3, z2_out, z2_in, s2_out, s2_in,
    x_sem, own_sem, w_send, w_recv, core_send, core_recv, z_send, z_recv, s_send, s_recv,
):
    columns = x.shape[0]
    size = w.shape[3] // 2
    rows = w_hbm.shape[2]
    blocks = w.shape[1]
    tiles = columns // TILE
    me_n = lax.axis_index("narrow")
    me_w = lax.axis_index("wide")
    sides = [me_w // stride % 2 for stride in strides]
    partners = [me_w + (1 - 2 * side) * stride for side, stride in zip(sides, strides)]

    def x_copy(half):
        span = pl.ds(half * 2 * size, 2 * size)
        return pltpu.make_async_copy(x_hbm.at[:, span], x.at[:, span], x_sem.at[half])

    def own_copy(level, block):
        span = pl.ds(pl.multiple_of(me_n * rows, rows), rows)
        return pltpu.make_async_copy(
            w_hbm.at[level, block], w.at[level, block, span], own_sem.at[level, block]
        )

    def weight_copy(level, block, k, owner):
        span = pl.ds(pl.multiple_of(owner * rows, rows), rows)
        return pltpu.make_async_remote_copy(
            src_ref=w_hbm.at[level, block],
            dst_ref=w.at[level, block, span],
            send_sem=w_send.at[level, block, k - 1],
            recv_sem=w_recv.at[level, block, k - 1],
            device_id={"narrow": lax.rem(me_n + k, peers)},
            device_id_type=MESH,
        )

    def send_weight(position):
        if position < len(WEIGHT_ORDER):
            level, block = WEIGHT_ORDER[position]
            for k in range(1, peers):
                weight_copy(level, block, k, me_n).start()

    def core_copy(block):
        return pltpu.make_async_remote_copy(
            src_ref=l1.at[block], dst_ref=l1_in.at[block],
            send_sem=core_send.at[block], recv_sem=core_recv.at[block],
            device_id={"wide": partners[0]}, device_id_type=MESH,
        )

    def code_copies(level, block, tile):
        source, target = ((z1_out, z1_in), (z2_out, z2_in))[level]
        s_source, s_target = ((s1_out, s1_in), (s2_out, s2_in))[level]
        partner = partners[level + 1]
        return (
            pltpu.make_async_remote_copy(
                src_ref=s_source.at[block, tile], dst_ref=s_target.at[block, tile],
                send_sem=s_send.at[level, block, tile], recv_sem=s_recv.at[level, block, tile],
                device_id={"wide": partner}, device_id_type=MESH,
            ),
            pltpu.make_async_remote_copy(
                src_ref=source.at[block, at_tile(tile)], dst_ref=target.at[block, at_tile(tile)],
                send_sem=z_send.at[level, block, tile], recv_sem=z_recv.at[level, block, tile],
                device_id={"wide": partner}, device_id_type=MESH,
            ),
        )

    def product(level, block, first, second, side, finish):
        def step(tile, carry):
            total = None
            for part, half in ((first, side), (second, 1 - side)):
                start = half * size
                if not isinstance(half, int):
                    start = pl.multiple_of(start, size)
                matrix = w[level, block, :, pl.ds(start, size)]
                lhs = jnp.concatenate(part(tile), axis=0)
                term = lax.dot_general(
                    lhs, matrix, (((1,), (1,)), ((), ())), preferred_element_type=F32
                )
                total = term if total is None else total + term
            finish(tile, total[:TILE] + total[TILE:])
            return carry

        lax.fori_loop(0, tiles, step, 0)

    def at_tile(tile):
        return pl.ds(pl.multiple_of(tile * TILE, TILE), TILE)

    def from_x(block):
        return lambda tile: split(x[at_tile(tile), pl.ds(block * size, size)])

    def from_pair(ref, block):
        return lambda tile: (ref[block, 0, at_tile(tile)], ref[block, 1, at_tile(tile)])

    def from_code(level, block):
        ref, scales = ((z1_in, s1_in), (z2_in, s2_in))[level]

        def load(tile):
            for copy in code_copies(level, block, tile):
                copy.wait_recv()
            return split(decode(ref[block, at_tile(tile)], scales[block, tile]))

        return load

    def to_pair(ref, block):
        def finish(tile, value):
            high, low = split(value)
            ref[block, 0, at_tile(tile)] = high
            ref[block, 1, at_tile(tile)] = low

        return finish

    def to_code(level, block):
        keep = to_pair((l2, l3)[level], block)
        code_ref, scale_ref = ((z1_out, s1_out), (z2_out, s2_out))[level]

        def finish(tile, value):
            keep(tile, value)
            code, scale = encode(value)
            code_ref[block, at_tile(tile)] = code
            scale_ref[block, tile] = scale
            for copy in code_copies(level, block, tile):
                copy.start()

        return finish

    def to_out(block):
        def finish(tile, value):
            out[at_tile(tile), pl.ds(block * size, size)] = value

        return finish

    for half in range(blocks // 2):
        x_copy(half).start()
    for level, block in WEIGHT_ORDER:
        own_copy(level, block).start()

    barrier = pltpu.get_barrier_semaphore()
    for k in range(1, peers):
        pl.semaphore_signal(
            barrier, inc=1, device_id={"narrow": lax.rem(me_n + k, peers)}, device_id_type=MESH
        )
    for partner in partners:
        pl.semaphore_signal(barrier, inc=1, device_id={"wide": partner}, device_id_type=MESH)
    pl.semaphore_wait(barrier, peers - 1 + len(partners))

    for position in range(WINDOW):
        send_weight(position)

    arrived = [0]

    def need_weight(level, block):
        while (level, block) in WEIGHT_ORDER[arrived[0]:]:
            next_level, next_block = WEIGHT_ORDER[arrived[0]]
            own_copy(next_level, next_block).wait()
            for k in range(1, peers):
                weight_copy(
                    next_level, next_block, k, lax.rem(me_n + peers - k, peers)
                ).wait_recv()
            send_weight(arrived[0] + WINDOW)
            arrived[0] += 1

    x_ready = set()
    for level, block in COMPUTE_ORDER:
        if level == 0 and block // 2 not in x_ready:
            x_copy(block // 2).wait()
            x_ready.add(block // 2)
        need_weight(level, block)
        if level < 2:
            stride = 1 << level
            low = block - block // stride % 2 * stride
            high = low + stride
        if level == 0:
            product(level, block, from_x(low), from_x(high), 0, to_pair(l0, block))
        elif level == 1:
            product(level, block, from_pair(l0, low), from_pair(l0, high), 0, to_pair(l1, block))
            core_copy(block).start()
        elif level == 2:
            core_copy(block).wait_recv()
            product(
                level, block, from_pair(l1, block), from_pair(l1_in, block), sides[0],
                to_code(0, block),
            )
        elif level == 3:
            product(
                level, block, from_pair(l2, block), from_code(0, block), sides[1],
                to_code(1, block),
            )
        else:
            product(
                level, block, from_pair(l3, block), from_code(1, block), sides[2], to_out(block)
            )

    for level, block in WEIGHT_ORDER:
        for k in range(1, peers):
            weight_copy(level, block, k, me_n).wait_send()
    for block in range(blocks):
        core_copy(block).wait_send()
        for level in range(2):
            for tile in range(tiles):
                for copy in code_copies(level, block, tile):
                    copy.wait_send()


def on_device(vectors, weights):
    columns, coeffs = vectors.shape
    levels, blocks, rows, depth = weights.shape
    size = depth // 2
    peers = lax.axis_size("narrow")
    wide_top = lax.axis_size("wide").bit_length() - 1
    strides = [1 << bit for bit in (0, wide_top // 2, wide_top - 1)]
    tiles = columns // TILE
    pair = pltpu.VMEM((blocks, 2, columns, size), BF16)
    code = pltpu.VMEM((blocks, columns, size), BF16)
    scale = pltpu.VMEM((blocks, tiles, 1, size), F32)
    dma = pltpu.SemaphoreType.DMA
    return pl.pallas_call(
        functools.partial(kernel, peers, strides),
        out_shape=pltpu.VMEM((columns, coeffs), F32),
        in_specs=[pl.BlockSpec(memory_space=pltpu.HBM)] * 2,
        out_specs=pl.BlockSpec(memory_space=pltpu.VMEM),
        scratch_shapes=[
            pltpu.VMEM((columns, coeffs), F32),
            pltpu.VMEM((levels, blocks, size, depth), BF16),
            pair, pair, pair, pair,
            code, code, scale, scale,
            pair,
            code, code, scale, scale,
            dma((blocks // 2,)),
            dma((levels, blocks)),
            dma((levels, blocks, max(peers - 1, 1))),
            dma((levels, blocks, max(peers - 1, 1))),
            dma((blocks,)),
            dma((blocks,)),
            dma((2, blocks, tiles)),
            dma((2, blocks, tiles)),
            dma((2, blocks, tiles)),
            dma((2, blocks, tiles)),
        ],
        compiler_params=pltpu.CompilerParams(
            collective_id=0, has_side_effects=True, vmem_limit_bytes=40 * 1024 * 1024
        ),
    )(vectors, weights)


def solution(mesh):
    placed = (P("narrow", "wide"), P(None, "wide", "narrow", None))
    return jax.shard_map(
        on_device, mesh=mesh, in_specs=placed, out_specs=P("narrow", "wide"), check_vma=False
    )
```
